32 devices in a mesh: dp: 1 (over z), tp: 4 (over y), ep: 8 (over x, core).
Axes of the slice: x: 4, y: 4, z: 1, core: 2. Of those that a mesh axis runs over, the one named last changes fastest.
The devices are a block of a 4x4x8 slice.
Arguments:
- x: bfloat16 [16384, 1536], P(('dp', 'ep'))
- idx: int32 [16384, 8], P(('dp', 'ep'))
- gates: float32 [16384, 8], P(('dp', 'ep'))
- w1: bfloat16 [40, 1536, 512], P('ep', None, 'tp')
- w2: bfloat16 [40, 512, 1536], P('ep', 'tp')
Outputs:
- output: bfloat16 [16384, 1536], P(('dp', 'ep', 'tp'))
All inputs are finite; a program needn't handle non-finite values.
Results may differ from the reference program's by a relative error of at most 0.001.
Values are sent between devices in bfloat16 or wider.
A program may use at most 768 MiB of HBM per device.

```python
import math
import jax
import jax.numpy as jnp
from jax import lax

EP = 8
TP = 4
T = 2048
H = 1536
F = 512
E = 40
K = 8
CAP = 128

S = T // TP
NSRC = EP * TP


def setup_inputs(seed: int = 0, part: int = 0) -> dict:
    key = jax.random.key(seed)
    kw1, kw2, kp = jax.random.split(key, 3)
    kx, kpop, kg, kgate, ksrc = jax.random.split(jax.random.fold_in(kp, part), 5)
    x = jax.random.normal(kx, (EP * T, H), jnp.float32).astype(jnp.bfloat16)
    pop = jax.random.randint(kpop, (E,), 0, 1 << 18, jnp.int32)
    src = jnp.repeat(jax.random.randint(ksrc, (NSRC, E), 0, 1 << 17, jnp.int32), S, axis=0)
    noise = jax.random.randint(kg, (EP * T, E), 0, 1 << 20, jnp.int32)
    score = (noise + pop[None, :] + src) * E + jnp.arange(E, dtype=jnp.int32)[None, :]
    idx = lax.top_k(score, K)[1].astype(jnp.int32)
    gates = jax.random.uniform(kgate, (EP * T, K), jnp.float32, minval=0.4, maxval=1.2) / math.sqrt(K)
    w1 = (jax.random.normal(kw1, (E, H, F), jnp.float32) / math.sqrt(H)).astype(jnp.bfloat16)
    w2 = (jax.random.normal(kw2, (E, F, H), jnp.float32) / math.sqrt(F)).astype(jnp.bfloat16)
    return {"x": x, "idx": idx, "gates": gates, "w1": w1, "w2": w2}


def slots_of(ids):
    flat = ids.reshape(S * K)
    oh = (flat[:, None] == jnp.arange(E, dtype=jnp.int32)[None, :]).astype(jnp.int32)
    slot = jnp.sum((jnp.cumsum(oh, axis=0) - 1) * oh, axis=1)
    return flat, slot


def reference(x, idx, gates, w1, w2):
    xs = x.reshape(NSRC, S, H)
    flat, slot = jax.vmap(slots_of)(idx.reshape(NSRC, S, K))
    wts = jnp.where(slot < CAP, gates.reshape(NSRC, S * K), 0.0)
    tok = jnp.arange(S * K) // K

    def fill(args):
        xv, fv, sv = args
        return jnp.zeros((E, CAP, H), x.dtype).at[fv, sv].set(xv[tok], mode="drop")

    buf = lax.map(fill, (xs, flat, slot))

    def expert(args):
        b, a1, a2 = args
        z = jnp.dot(b.reshape(NSRC * CAP, H), a1, preferred_element_type=jnp.float32)
        hb = jax.nn.gelu(z).astype(jnp.bfloat16)
        o = jnp.dot(hb, a2, preferred_element_type=jnp.float32).astype(jnp.bfloat16)
        return o.reshape(NSRC, CAP, H)

    out = jnp.swapaxes(lax.map(expert, (jnp.swapaxes(buf, 0, 1), w1, w2)), 0, 1)

    def combine(args):
        ov, fv, sv, wv = args
        rows = ov[fv, jnp.minimum(sv, CAP - 1)].astype(jnp.float32)
        return jnp.sum((rows * wv[:, None]).reshape(S, K, H), axis=1)

    y = lax.map(combine, (out, flat, slot, wts))
    return y.reshape(NSRC * S, H).astype(jnp.bfloat16)
```

```python
import jax
import jax.numpy as jnp
from jax import lax
from jax.sharding import PartitionSpec as P


def kept_gates(ids, gs, n_exp, cap):
    s = ids.shape[0]
    hit = ids[:, :, None] == jnp.arange(n_exp, dtype=jnp.int32)[None, None, :]
    one = jnp.sum(hit.astype(jnp.float32), axis=1)
    dense = jnp.sum(jnp.where(hit, gs[:, :, None], 0.0), axis=1)
    earlier = (jnp.arange(s)[:, None] > jnp.arange(s)[None, :]).astype(jnp.bfloat16)
    slot = jnp.dot(earlier, one.astype(jnp.bfloat16), preferred_element_type=jnp.float32)
    return jnp.where(slot < cap, dense, 0.0)


def solution(mesh):
    ntp = mesh.shape["tp"]
    nep = mesh.shape["ep"]

    def body(x, idx, gates, w1, w2):
        t_n, h = x.shape
        el = w1.shape[0]
        n_exp = el * nep
        k = idx.shape[1]
        s = t_n // ntp
        cap = 8 * ((5 * k * s + 32 * n_exp - 1) // (32 * n_exp))
        j = lax.axis_index("tp")
        i = lax.axis_index("ep")
        xs = lax.dynamic_slice_in_dim(x, j * s, s, 0)
        ids = lax.dynamic_slice_in_dim(idx, j * s, s, 0)
        gs = lax.dynamic_slice_in_dim(gates, j * s, s, 0)
        w1f = lax.all_gather(w1, "tp", axis=2, tiled=True)
        w2f = lax.all_gather(w2, "tp", axis=1, tiled=True)
        xa = lax.all_gather(xs, "ep", axis=0, tiled=True)
        g = kept_gates(ids, gs, n_exp, cap)
        ga = lax.all_gather(g, "ep", axis=0, tiled=True)
        ge = lax.dynamic_slice_in_dim(ga, i * el, el, 1)
        acc = jnp.zeros((nep * s, h), jnp.float32)
        for e in range(el):
            col = ge[:, e][:, None]
            z = jnp.dot(xa, w1f[e], preferred_element_type=jnp.float32)
            a = jnp.where(col != 0.0, jax.nn.gelu(z), 0.0).astype(jnp.bfloat16)
            o = jnp.dot(a, w2f[e], preferred_element_type=jnp.float32).astype(jnp.bfloat16)
            acc = acc + o.astype(jnp.float32) * col
        y = lax.psum_scatter(acc, "ep", scatter_dimension=0, tiled=True)
        return y.astype(jnp.bfloat16)

    row = P(("dp", "ep"), None)
    return jax.shard_map(
        body,
        mesh=mesh,
        in_specs=(row, row, row, P("ep", None, "tp"), P("ep", "tp", None)),
        out_specs=P(("dp", "ep", "tp"), None),
        check_vma=False,
    )
```

```python
import functools

import jax
import jax.numpy as jnp
from jax import lax
from jax.experimental import pallas as pl
from jax.experimental.pallas import tpu as pltpu
from jax.sharding import PartitionSpec as P


MESH = pl.DeviceIdType.MESH
CORES = 2
CHUNK = 256
SLOTS = 4
RING = ((1, 2), (3, 3), (2, 1), (0, 0))


def kept_gates(ids, gs, n_exp, cap):
    s = ids.shape[0]
    hit = ids[:, :, None] == jnp.arange(n_exp, dtype=jnp.int32)[None, None, :]
    one = jnp.sum(hit.astype(jnp.float32), axis=1)
    dense = jnp.sum(jnp.where(hit, gs[:, :, None], 0.0), axis=1)
    earlier = (jnp.arange(s)[:, None] > jnp.arange(s)[None, :]).astype(jnp.bfloat16)
    slot = jnp.dot(earlier, one.astype(jnp.bfloat16), preferred_element_type=jnp.float32)
    return jnp.where(slot < cap, dense, 0.0)


def kernel(x_ref, gt_ref, w1_ref, w2_ref, y_ref, w2f, xb, gtb, gb, wb, ab, rb, part,
           xl_sem, x_snd, x_rcv, g_snd, g_rcv, l1_sem, w1_snd, w1_rcv, w2_snd, w2_rcv,
           ld_sem, rs_snd, rs_rcv, *, ntp, nep):
    s, h = xb.shape[1:]
    el, nb = w1_ref.shape[0], w1_ref.shape[1]
    fs = w1_ref.shape[3]
    kb = ntp * fs
    hr = s // 2
    nq = h // CHUNK
    nx = nep // CORES

    ep, y = lax.axis_index("ep"), lax.axis_index("tp")
    core, cx = lax.rem(ep, CORES), lax.div(ep, CORES)

    def along_x(d):
        return {"ep": lax.rem(cx + d, nx) * CORES + core}

    right, left, across = along_x(1), along_x(nx - 1), along_x(2)
    up, down = {"tp": lax.rem(y + 1, ntp)}, {"tp": lax.rem(y + ntp - 1, ntp)}
    peer = {"ep": cx * CORES + (CORES - 1 - core)}

    barrier = pltpu.get_barrier_semaphore()
    for dev in (right, left, across, up, down, peer):
        pl.semaphore_signal(barrier, inc=1, device_id=dev, device_id_type=MESH)
    pl.semaphore_wait(barrier, 6)

    def remote(src, dst, snd, rcv, dev):
        return pltpu.make_async_remote_copy(
            src_ref=src, dst_ref=dst, send_sem=snd, recv_sem=rcv, device_id=dev,
            device_id_type=MESH)

    x0 = pl.multiple_of(y * s, s)
    lo, hi = pl.ds(0, hr), pl.ds(hr, hr)

    def cx_copy(kind):
        src = (x_ref.at[pl.ds(x0, hr)], x_ref.at[pl.ds(x0 + hr, hr)], x_ref.at[pl.ds(x0 + hr, hr)],
               x_ref.at[pl.ds(x0, hr)], xb.at[1, lo], xb.at[2, hi])[kind]
        dst = (xb.at[1, lo], xb.at[1, hi], xb.at[2, hi], xb.at[2, lo], xb.at[3, lo], xb.at[3, hi])[kind]
        dev = (right, right, left, left, right, left)[kind]
        return remote(src, dst, x_snd.at[kind], x_rcv.at[kind], dev)

    def g_copy(kind):
        far, slot, dev = ((1, 1, right), (3, 2, left), (2, 3, across))[kind]
        return remote(gt_ref.at[far], gtb.at[slot], g_snd.at[kind], g_rcv.at[kind], dev)

    h1 = wb.shape[1] // 2
    mine, others = pl.ds(0, fs), pl.ds(fs, fs)
    whole1, a1, b1 = pl.ds(0, 2 * h1), pl.ds(0, h1), pl.ds(h1, h1)

    def w1_copy(kind, e):
        def at(slot, rows, lanes):
            return wb.at[pl.ds((e * ntp + slot) * nb, nb), rows, lanes]

        src, dst, dev = (
            lambda: (w1_ref.at[e], at(1, whole1, mine), up),
            lambda: (w1_ref.at[e], at(2, whole1, mine), down),
            lambda: (w1_ref.at[e], at(0, whole1, others), peer),
            lambda: (at(1, a1, mine), at(3, a1, mine), up),
            lambda: (at(2, b1, mine), at(3, b1, mine), down),
            lambda: (at(1, whole1, mine), at(1, whole1, others), peer),
            lambda: (at(2, whole1, mine), at(2, whole1, others), peer),
            lambda: (at(3, a1, mine), at(3, a1, others), peer),
            lambda: (at(3, b1, mine), at(3, b1, others), peer),
        )[kind]()
        return remote(src, dst, w1_snd.at[kind, e], w1_rcv.at[kind, e], dev)

    def w2_copy(kind, q):
        def at(slot, off, n, cs):
            return w2f.at[pl.ds((q * CORES + cs) * el, el), pl.ds(slot * fs + off, n), :]

        own = w2_ref.at[:, :, pl.ds(q * CHUNK, CHUNK)]
        hf = fs // 2
        src, dst, dev = (
            lambda: (own, at(1, 0, fs, 0), up),
            lambda: (own, at(2, 0, fs, 0), down),
            lambda: (own, at(0, 0, fs, 1), peer),
            lambda: (at(1, 0, hf, 0), at(3, 0, hf, 0), up),
            lambda: (at(2, hf, hf, 0), at(3, hf, hf, 0), down),
            lambda: (at(1, 0, fs, 0), at(1, 0, fs, 1), peer),
            lambda: (at(2, 0, fs, 0), at(2, 0, fs, 1), peer),
            lambda: (at(3, 0, hf, 0), at(3, 0, hf, 1), peer),
            lambda: (at(3, hf, hf, 0), at(3, hf, hf, 1), peer),
        )[kind]()
        return remote(src, dst, w2_snd.at[kind, q], w2_rcv.at[kind, q], dev)

    def start(copy, kinds, n):
        for kind in kinds:
            copy(kind, n).start()

    def arrived(copy, kinds, n):
        for kind in kinds:
            copy(kind, n).wait_recv()

    def near(copy, n):
        arrived(copy, (0, 1), n)
        start(copy, (3, 4, 5, 6), n)

    def far(copy, n):
        arrived(copy, (3, 4), n)
        start(copy, (7, 8), n)

    x_own = pltpu.make_async_copy(x_ref.at[pl.ds(x0, s)], xb.at[0], xl_sem.at[0])
    g_own = pltpu.make_async_copy(gt_ref.at[0], gtb.at[0], xl_sem.at[1])

    def w1_own(e):
        return pltpu.make_async_copy(
            w1_ref.at[e], wb.at[pl.ds(e * ntp * nb, nb), :, mine], l1_sem.at[e])

    start(w1_copy, (0, 1, 2), 0)
    for kind in range(4):
        cx_copy(kind).start()
    x_own.start()
    w1_own(0).start()
    for e in range(1, el):
        start(w1_copy, (0, 1, 2), e)
        w1_own(e).start()
    for kind in range(3):
        g_copy(kind).start()
    g_own.start()

    def hidden(b0, n, e, slot):
        w = wb[pl.ds((e * ntp + slot) * nb, nb)].reshape(h, CORES * fs)
        z = jnp.dot(xb[b0:b0 + n].reshape(n * s, h), w, preferred_element_type=jnp.float32)
        cdf = 0.5 * (1.0 + jnp.tanh(0.7978845608028654 * (z + 0.044715 * (z * z * z))))
        a = (z * cdf).astype(jnp.bfloat16)
        cols = pl.ds(pl.multiple_of(slot * fs, fs), fs)
        for b in range(n):
            rows = a[b * s:(b + 1) * s]
            for cs in range(CORES):
                ab[(b0 + b) * CORES * el + cs * el + e, :, cols] = rows[:, cs * fs:(cs + 1) * fs]

    def hiddens(b0, n, e0, e1, s0, s1):
        def step(i, _):
            hidden(b0, n, e0 + lax.div(i, s1 - s0), s0 + lax.rem(i, s1 - s0))
            return 0
        lax.fori_loop(0, (e1 - e0) * (s1 - s0), step, 0)

    for e in range(el):
        w1_own(e).wait()
        w1_copy(2, e).wait_recv()
    x_own.wait()
    hiddens(0, 1, 0, el, 0, 1)

    late = max(el - 2, 0)
    for e in range(el):
        if e == late:
            start(w2_copy, (0, 1, 2), 0)
        near(w1_copy, e)
        if e == min(1, el - 1):
            cx_copy(0).wait_recv()
            cx_copy(2).wait_recv()
            cx_copy(4).start()
            cx_copy(5).start()
        if e == 0:
            g_own.wait()
            for kind in range(3):
                g_copy(kind).wait_recv()
            for b in range(4):
                g = gtb[b]
                pad = jnp.zeros((128 - g.shape[0], s), jnp.float32)
                gb[b] = jnp.transpose(jnp.concatenate([g, pad], axis=0))
        if e >= 1:
            arrived(w1_copy, (5, 6), e - 1)
            hiddens(0, 1, e - 1, e, 1, 3)
        if e == late:
            cx_copy(1).wait_recv()
            cx_copy(3).wait_recv()
            hiddens(1, 2, 0, late, 0, 3)
    arrived(w1_copy, (5, 6), el - 1)
    hiddens(0, 1, el - 1, el, 1, 3)
    far(w1_copy, 0)
    hiddens(1, 2, late, el, 0, 3)
    far(w1_copy, 1)
    cx_copy(4).wait_recv()
    cx_copy(5).wait_recv()
    hiddens(3, 1, 0, el, 0, 3)
    for e in range(el):
        if e + 2 == late:
            near(w2_copy, 0)
            start(w2_copy, (0, 1, 2), 1)
        if e + 2 < el:
            far(w1_copy, e + 2)
        arrived(w1_copy, (7, 8), e)
        hiddens(0, 2, e, e + 1, 3, 4)
        hiddens(2, 2, e, e + 1, 3, 4)
    if late < 2:
        near(w2_copy, 0)
        start(w2_copy, (0, 1, 2), 1)

    def loads(q):
        n0 = q * CORES * el
        return (
            pltpu.make_async_copy(w2_ref.at[:, :, pl.ds(q * CHUNK, CHUNK)],
                                  wb.at[pl.ds(n0, el), pl.ds(0, fs), :], ld_sem.at[0, q]),
            pltpu.make_async_copy(w2f.at[pl.ds(n0, el), pl.ds(fs, kb - fs), :],
                                  wb.at[pl.ds(n0, el), pl.ds(fs, kb - fs), :], ld_sem.at[1, q]),
            pltpu.make_async_copy(w2f.at[pl.ds(n0 + el, el)], wb.at[pl.ds(n0 + el, el)],
                                  ld_sem.at[2, q]),
        )

    def load(q):
        arrived(w2_copy, (2, 5, 6, 7, 8), q)
        for copy in loads(q):
            copy.start()

    def loaded(q):
        for copy in loads(q):
            copy.wait()

    lane = lax.broadcasted_iota(jnp.int32, (s, 128), 1)

    def halves(ref, r, l, off):
        if r == l:
            return ref[r * off[0] + off[1]]
        return jnp.concatenate(
            [ref[r * off[0] + off[1], 0:hr], ref[l * off[0] + off[1], hr:s]], axis=0)

    def outputs(q, step, k):
        r, l = RING[step]

        def gated(e, cs):
            n = cs * el + e
            o = jnp.dot(halves(ab, r, l, (CORES * el, n)), wb[q * CORES * el + n],
                        preferred_element_type=jnp.float32)
            o = o.astype(jnp.bfloat16).astype(jnp.float32)
            col = jnp.sum(jnp.where(lane == n, halves(gb, r, l, (1, 0)), 0.0), axis=1, keepdims=True)
            return jnp.where(col != 0.0, o * col, 0.0)

        part[k] = gated(0, 0) + gated(0, 1)

        def more(e, _):
            part[k] = part[k] + (gated(e, 0) + gated(e, 1))
            return 0
        lax.fori_loop(1, el, more, 0)

    def ring(q, step, k):
        return (remote(part.at[k, lo], rb.at[0, q, step], rs_snd.at[0, q, step], rs_rcv.at[0, q, step], right),
                remote(part.at[k, hi], rb.at[1, q, step], rs_snd.at[1, q, step], rs_rcv.at[1, q, step], left))

    def add_arrived(q, step, k):
        for copy in ring(q, step - 1, k):
            copy.wait_recv()
        return (part[k, 0:hr] + rb[0, q, step - 1], part[k, hr:s] + rb[1, q, step - 1])

    sent = []

    def hop(q, step):
        n = len(sent)
        k = n % SLOTS
        if n >= SLOTS:
            for copy in sent[n - SLOTS]:
                copy.wait_send()
        outputs(q, step, k)
        if step:
            top, bottom = add_arrived(q, step, k)
            part[k, 0:hr] = top
            part[k, hr:s] = bottom
        sent.append(ring(q, step, k))
        for copy in sent[-1]:
            copy.start()

    def finish(q):
        outputs(q, 3, SLOTS)
        top, bottom = add_arrived(q, 3, SLOTS)
        cols = pl.ds(q * CHUNK, CHUNK)
        y_ref[0:hr, cols] = top.astype(y_ref.dtype)
        y_ref[hr:s, cols] = bottom.astype(y_ref.dtype)

    todo = {}

    def before(n, fn, *args):
        todo.setdefault(n, []).append(functools.partial(fn, *args))

    def near2(q):
        near(w2_copy, q)
        if q + 1 < nq:
            start(w2_copy, (0, 1, 2), q + 1)

    def w1_sent():
        for kind in range(9):
            for e in range(el):
                w1_copy(kind, e).wait_send()

    before(0, far, w2_copy, 0)
    before(0, w1_sent)
    before(0, load, 0)
    before(1, near2, 1)
    before(1, far, w2_copy, 1)
    before(1, load, 1)
    for q in range(2, nq):
        before(2 * q - 2, near2, q)
        before(2 * q - 1, far, w2_copy, q)
        before(max(2 * q + 1, 6 * (q // 2) - 1), load, q)

    order = []
    for p in range(nq // 2):
        pair = (2 * p, 2 * p + 1)
        for step in range(3):
            for q in pair:
                order.append((q, step))
    for n, (q, step) in enumerate(order):
        for fn in todo.get(n, ()):
            fn()
        if step == 0:
            loaded(q)
        hop(q, step)
        if step == 0 and q >= 2:
            finish(q - 2)
    for q in (nq - 2, nq - 1):
        finish(q)

    for copies in sent[-SLOTS:]:
        for copy in copies:
            copy.wait_send()
    for kind in range(6):
        cx_copy(kind).wait_send()
    for kind in range(3):
        g_copy(kind).wait_send()
    for kind in range(9):
        for q in range(nq):
            w2_copy(kind, q).wait_send()


def solution(mesh):
    ntp = mesh.shape["tp"]
    nep = mesh.shape["ep"]
    nx = nep // CORES

    def body(x, idx, gates, w1, w2):
        t_n, h = x.shape
        el, fs = w1.shape[0], w1.shape[2]
        n_exp = el * nep
        k = idx.shape[1]
        s = t_n // ntp
        cap = 8 * ((5 * k * s + 32 * n_exp - 1) // (32 * n_exp))
        kb = ntp * fs
        nb = h // kb
        nq = h // CHUNK
        j = lax.axis_index("tp")
        i = lax.axis_index("ep")
        ids = lax.dynamic_slice_in_dim(idx, j * s, s, 0)
        gs = lax.dynamic_slice_in_dim(gates, j * s, s, 0)
        g = kept_gates(ids, gs, n_exp, cap)
        gt = g.T.reshape(nx, CORES, el, s)
        gt = jnp.where(i % CORES == 0, gt, gt[:, ::-1])
        gt = jnp.roll(gt, -(i // CORES), axis=0).reshape(nx, CORES * el, s)
        rows = -(-CORES * el // 8) * 8
        gt = jnp.pad(gt, ((0, 0), (0, rows - CORES * el), (0, 0)))

        bf16, f32, dma = jnp.bfloat16, jnp.float32, pltpu.SemaphoreType.DMA
        any_space = pl.BlockSpec(memory_space=pl.ANY)
        y, _ = pl.pallas_call(
            functools.partial(kernel, ntp=ntp, nep=nep),
            out_shape=(jax.ShapeDtypeStruct((s, h), bf16),
                       jax.ShapeDtypeStruct((nq * CORES * el, kb, CHUNK), bf16)),
            in_specs=[any_space] * 4,
            out_specs=(pl.BlockSpec(memory_space=pltpu.VMEM), any_space),
            scratch_shapes=[
                pltpu.VMEM((4, s, h), bf16),
                pltpu.VMEM((4, rows, s), f32),
                pltpu.VMEM((4, s, 128), f32),
                pltpu.VMEM((nq * CORES * el, kb, CHUNK), bf16),
                pltpu.VMEM((4 * CORES * el, s, kb), bf16),
                pltpu.VMEM((2, nq, 3, s // 2, CHUNK), f32),
                pltpu.VMEM((SLOTS + 1, s, CHUNK), f32),
                dma((2,)), dma((6,)), dma((6,)), dma((3,)), dma((3,)), dma((el,)),
                dma((9, el)), dma((9, el)), dma((9, nq)), dma((9, nq)),
                dma((3, nq)), dma((2, nq, 3)), dma((2, nq, 3)),
            ],
            compiler_params=pltpu.CompilerParams(
                collective_id=0, has_side_effects=True, vmem_limit_bytes=67_000_000),
        )(x, gt, w1.reshape(el, nb, kb, fs), w2)
        return y

    row = P(("dp", "ep"), None)
    return jax.shard_map(
        body,
        mesh=mesh,
        in_specs=(row, row, row, P("ep", None, "tp"), P("ep", "tp", None)),
        out_specs=P(("dp", "ep", "tp"), None),
        check_vma=False,
    )
```

```python
import functools

import jax
import jax.numpy as jnp
from jax import lax
from jax.experimental import pallas as pl
from jax.experimental.pallas import tpu as pltpu
from jax.sharding import PartitionSpec as P


MESH = pl.DeviceIdType.MESH
CORES = 2
CHUNK = 256
SLOTS = 4
DIRECT = 2
RING = ((1, 2), (3, 3), (2, 1), (0, 0))
PROGRAM = (
    ("N1", 0), ("N1", 1), ("X1",), ("G",), ("H", 0, 1, 0, 2, 0), ("N1", 2), ("W", 0), ("N1", 3),
    ("X2",), ("H", 1, 2, 0, 3, 0), ("N1", 4), ("H", 1, 2, 3, 5, 0), ("F1", 0), ("F1", 1),
    ("H", 0, 1, 2, 5, 0), ("F1", 2), ("H", 1, 2, 0, 2, 1), ("X3",), ("H", 3, 1, 0, 2, 0), ("N2", 0),
    ("W", 1), ("H", 3, 1, 2, 5, 0), ("F1", 3), ("H", 1, 2, 2, 4, 1), ("F1", 4),
    ("H", 1, 2, 4, 5, 1), ("F2", 0), ("L", 0), ("R", 0, 0), ("H", 3, 1, 0, 5, 1), ("N2", 1),
    ("W", 2), ("H", 0, 1, 0, 5, 1), ("R", 0, 1), ("F2", 1), ("L", 1), ("R", 1, 0), ("N2", 2),
    ("W", 3), ("R", 0, 2), ("F2", 2), ("R", 1, 1), ("L", 2), ("R", 2, 0), ("E", 0), ("N2", 3),
    ("W", 4), ("R", 1, 2), ("F2", 3), ("R", 2, 1), ("L", 3), ("N2", 4), ("W", 5), ("R", 3, 0),
    ("R", 2, 2), ("F2", 4), ("E", 1), ("R", 3, 1), ("N2", 5), ("L", 4), ("R", 4, 0), ("E", 2),
    ("F2", 5), ("R", 3, 2), ("L", 5), ("R", 5, 0), ("R", 4, 1), ("E", 3), ("R", 5, 1), ("R", 4, 2),
    ("R", 5, 2), ("E", 4), ("E", 5),
)


def kernel(x_ref, idx_ref, gates_ref, w1_ref, w2_ref, y_ref, w2f, xb, ids, gs, gto, gtb, gb, wb, wv,
           ab, rb, part, xl_sem, x_snd, x_rcv, g_snd, g_rcv, l1_sem, w1_snd, w1_rcv, w2_snd, w2_rcv,
           ld_sem, rs_snd, rs_rcv, *, ntp, nep, cap):
    s, h = xb.shape[1:]
    el, nb = w1_ref.shape[0], w1_ref.shape[1]
    fs = w1_ref.shape[3]
    kb = ntp * fs
    hr = s // 2
    nq = h // CHUNK
    nx = nep // CORES

    ep, y = lax.axis_index("ep"), lax.axis_index("tp")
    core, cx = lax.rem(ep, CORES), lax.div(ep, CORES)

    def along_x(d):
        return {"ep": lax.rem(cx + d, nx) * CORES + core}

    right, left, across = along_x(1), along_x(nx - 1), along_x(2)
    up, down = {"tp": lax.rem(y + 1, ntp)}, {"tp": lax.rem(y + ntp - 1, ntp)}
    peer = {"ep": cx * CORES + (CORES - 1 - core)}

    barrier = pltpu.get_barrier_semaphore()
    for dev in (right, left, across, up, down, peer):
        pl.semaphore_signal(barrier, inc=1, device_id=dev, device_id_type=MESH)
    pl.semaphore_wait(barrier, 6)

    def remote(src, dst, snd, rcv, dev):
        return pltpu.make_async_remote_copy(
            src_ref=src, dst_ref=dst, send_sem=snd, recv_sem=rcv, device_id=dev,
            device_id_type=MESH)

    x0 = pl.multiple_of(y * s, s)
    lo, hi = pl.ds(0, hr), pl.ds(hr, hr)

    def cx_copy(kind):
        src = (x_ref.at[pl.ds(x0, hr)], x_ref.at[pl.ds(x0 + hr, hr)], x_ref.at[pl.ds(x0 + hr, hr)],
               x_ref.at[pl.ds(x0, hr)], xb.at[1, lo], xb.at[2, hi])[kind]
        dst = (xb.at[1, lo], xb.at[1, hi], xb.at[2, hi], xb.at[2, lo], xb.at[3, lo], xb.at[3, hi])[kind]
        dev = (right, right, left, left, right, left)[kind]
        return remote(src, dst, x_snd.at[kind], x_rcv.at[kind], dev)

    def g_copy(kind):
        far, slot, dev = ((1, 1, right), (3, 2, left), (2, 3, across))[kind]
        return remote(gto.at[far], gtb.at[slot], g_snd.at[kind], g_rcv.at[kind], dev)

    h1 = wb.shape[1] // 2
    mine, others = pl.ds(0, fs), pl.ds(fs, fs)
    whole1, a1, b1 = pl.ds(0, 2 * h1), pl.ds(0, h1), pl.ds(h1, h1)

    def w1_copy(kind, e):
        def at(slot, rows, lanes):
            return wb.at[pl.ds((e * ntp + slot) * nb, nb), rows, lanes]

        src, dst, dev = (
            lambda: (w1_ref.at[e], at(1, whole1, mine), up),
            lambda: (w1_ref.at[e], at(2, whole1, mine), down),
            lambda: (w1_ref.at[e], at(0, whole1, others), peer),
            lambda: (at(1, a1, mine), at(3, a1, mine), up),
            lambda: (at(2, b1, mine), at(3, b1, mine), down),
            lambda: (at(1, whole1, mine), at(1, whole1, others), peer),
            lambda: (at(2, whole1, mine), at(2, whole1, others), peer),
            lambda: (at(3, a1, mine), at(3, a1, others), peer),
            lambda: (at(3, b1, mine), at(3, b1, others), peer),
        )[kind]()
        return remote(src, dst, w1_snd.at[kind, e], w1_rcv.at[kind, e], dev)

    def w2_copy(kind, q):
        def at(slot, off, n, cs):
            buf, at_q = (wv, q) if q < DIRECT else (w2f, q - DIRECT)
            return buf.at[pl.ds((at_q * CORES + cs) * el, el), pl.ds(slot * fs + off, n), :]

        own = w2_ref.at[:, :, pl.ds(q * CHUNK, CHUNK)]
        hf = fs // 2
        src, dst, dev = (
            lambda: (own, at(1, 0, fs, 0), up),
            lambda: (own, at(2, 0, fs, 0), down),
            lambda: (own, at(0, 0, fs, 1), peer),
            lambda: (at(1, 0, hf, 0), at(3, 0, hf, 0), up),
            lambda: (at(2, hf, hf, 0), at(3, hf, hf, 0), down),
            lambda: (at(1, 0, fs, 0), at(1, 0, fs, 1), peer),
            lambda: (at(2, 0, fs, 0), at(2, 0, fs, 1), peer),
            lambda: (at(3, 0, hf, 0), at(3, 0, hf, 1), peer),
            lambda: (at(3, hf, hf, 0), at(3, hf, hf, 1), peer),
        )[kind]()
        return remote(src, dst, w2_snd.at[kind, q], w2_rcv.at[kind, q], dev)

    def start(copy, kinds, n):
        for kind in kinds:
            copy(kind, n).start()

    def arrived(copy, kinds, n):
        for kind in kinds:
            copy(kind, n).wait_recv()

    def near(copy, n):
        arrived(copy, (0, 1), n)
        start(copy, (3, 4, 5, 6), n)

    def far(copy, n):
        arrived(copy, (3, 4), n)
        start(copy, (7, 8), n)

    x_own = pltpu.make_async_copy(x_ref.at[pl.ds(x0, s)], xb.at[0], xl_sem.at[0])
    tokens = pl.ds(x0, s)
    idx_own = pltpu.make_async_copy(idx_ref.at[:, tokens], ids, xl_sem.at[1])
    gates_own = pltpu.make_async_copy(gates_ref.at[:, tokens], gs, xl_sem.at[2])

    def w2_own(q):
        return pltpu.make_async_copy(
            w2_ref.at[:, :, pl.ds(q * CHUNK, CHUNK)],
            wv.at[pl.ds(q * CORES * el, el), pl.ds(0, fs), :], ld_sem.at[0, q])

    def w1_own(e):
        return pltpu.make_async_copy(
            w1_ref.at[e], wb.at[pl.ds(e * ntp * nb, nb), :, mine], l1_sem.at[e])

    idx_own.start()
    gates_own.start()
    start(w1_copy, (0, 1, 2), 0)
    for kind in range(4):
        cx_copy(kind).start()
    x_own.start()
    w1_own(0).start()
    for e in range(1, el):
        start(w1_copy, (0, 1, 2), e)
        w1_own(e).start()
    for q in range(DIRECT):
        w2_own(q).start()

    def gates_out():
        idx_own.wait()
        gates_own.wait()
        v = ids[...]
        block = jnp.zeros(v.shape, jnp.int32)
        for m in range(1, nep):
            block = block + (v >= el * m).astype(jnp.int32)
        swap = jnp.where((block & 1) == core, 0, el)
        n = gto.shape[1]
        row = (((block >> 1) - cx + nx) & (nx - 1)) * n + swap + (v - el * block)
        rows = lax.broadcasted_iota(jnp.int32, (nx * n, s), 0)
        one = jnp.zeros((nx * n, s), jnp.float32)
        dense = jnp.zeros((nx * n, s), jnp.float32)
        for k in range(v.shape[0]):
            hit = rows == row[k:k + 1]
            one = one + jnp.where(hit, 1.0, 0.0)
            dense = dense + jnp.where(hit, gs[k:k + 1], 0.0)
        before = (lax.broadcasted_iota(jnp.int32, (s, s), 0)
                  < lax.broadcasted_iota(jnp.int32, (s, s), 1))
        slot = jnp.dot(one.astype(jnp.bfloat16), jnp.where(before, 1.0, 0.0).astype(jnp.bfloat16),
                       preferred_element_type=jnp.float32)
        kept = jnp.where(slot < cap, dense, 0.0).reshape(nx, n, s)
        gto[...] = kept
        gtb[0] = kept[0]
        for kind in range(3):
            g_copy(kind).start()

    def gates_in():
        for kind in range(3):
            g_copy(kind).wait_recv()
        for b in range(4):
            g = gtb[b]
            pad = jnp.zeros((128 - g.shape[0], s), jnp.float32)
            gb[b] = jnp.transpose(jnp.concatenate([g, pad], axis=0))

    def hidden(b0, n, e, slot):
        w = wb[pl.ds((e * ntp + slot) * nb, nb)].reshape(h, CORES * fs)
        z = jnp.dot(xb[b0:b0 + n].reshape(n * s, h), w, preferred_element_type=jnp.float32)
        t = jnp.tanh(z * (0.7978845608028654 + 0.035677408136300125 * (z * z)))
        a = ((0.5 * z) * (1.0 + t)).astype(jnp.bfloat16)
        cols = pl.ds(pl.multiple_of(slot * fs, fs), fs)
        for b in range(n):
            rows = a[b * s:(b + 1) * s]
            for cs in range(CORES):
                ab[(b0 + b) * CORES * el + cs * el + e, :, cols] = rows[:, cs * fs:(cs + 1) * fs]

    def hiddens(b0, n, e0, e1, s0, s1):
        def step(i, _):
            hidden(b0, n, e0 + lax.div(i, s1 - s0), s0 + lax.rem(i, s1 - s0))
            return 0
        lax.fori_loop(0, (e1 - e0) * (s1 - s0), step, 0)

    def loads(q):
        src, dst = (q - DIRECT) * CORES * el, (q - DIRECT) * CORES * el
        return (
            pltpu.make_async_copy(w2_ref.at[:, :, pl.ds(q * CHUNK, CHUNK)],
                                  wb.at[pl.ds(dst, el), pl.ds(0, fs), :], ld_sem.at[0, q]),
            pltpu.make_async_copy(w2f.at[pl.ds(src, el), pl.ds(fs, kb - fs), :],
                                  wb.at[pl.ds(dst, el), pl.ds(fs, kb - fs), :], ld_sem.at[1, q]),
            pltpu.make_async_copy(w2f.at[pl.ds(src + el, el)], wb.at[pl.ds(dst + el, el)],
                                  ld_sem.at[2, q]),
        )

    def load(q):
        arrived(w2_copy, (2, 5, 6, 7, 8), q)
        if q < DIRECT:
            w2_own(q).wait()
            return
        if q == DIRECT:
            for kind in range(9):
                for e in range(el):
                    w1_copy(kind, e).wait_send()
        for copy in loads(q):
            copy.start()

    def loaded(q):
        if q >= DIRECT:
            for copy in loads(q):
                copy.wait()

    lane = lax.broadcasted_iota(jnp.int32, (s, 128), 1)

    def halves(ref, r, l, off):
        if r == l:
            return ref[r * off[0] + off[1]]
        return jnp.concatenate(
            [ref[r * off[0] + off[1], 0:hr], ref[l * off[0] + off[1], hr:s]], axis=0)

    def outputs(q, step, k):
        r, l = RING[step]

        def gated(e, cs):
            n = cs * el + e
            w = wv[q * CORES * el + n] if q < DIRECT else wb[(q - DIRECT) * CORES * el + n]
            o = jnp.dot(halves(ab, r, l, (CORES * el, n)), w,
                        preferred_element_type=jnp.float32)
            o = o.astype(jnp.bfloat16).astype(jnp.float32)
            col = jnp.sum(jnp.where(lane == n, halves(gb, r, l, (1, 0)), 0.0), axis=1, keepdims=True)
            return jnp.where(col != 0.0, o * col, 0.0)

        part[k] = jnp.zeros((s, CHUNK), jnp.float32)

        def more(e, _):
            part[k] = part[k] + (gated(e, 0) + gated(e, 1))
            return 0
        lax.fori_loop(0, el, more, 0)

    def ring(q, step, k):
        return (remote(part.at[k, lo], rb.at[0, q, step], rs_snd.at[0, q, step], rs_rcv.at[0, q, step], right),
                remote(part.at[k, hi], rb.at[1, q, step], rs_snd.at[1, q, step], rs_rcv.at[1, q, step], left))

    def add_arrived(q, step, k):
        for copy in ring(q, step - 1, k):
            copy.wait_recv()
        return (part[k, 0:hr] + rb[0, q, step - 1], part[k, hr:s] + rb[1, q, step - 1])

    sent = []

    def hop(q, step):
        n = len(sent)
        k = n % SLOTS
        if n >= SLOTS:
            for copy in sent[n - SLOTS]:
                copy.wait_send()
        outputs(q, step, k)
        if step:
            top, bottom = add_arrived(q, step, k)
            part[k, 0:hr] = top
            part[k, hr:s] = bottom
        sent.append(ring(q, step, k))
        for copy in sent[-1]:
            copy.start()

    def finish(q):
        outputs(q, 3, SLOTS)
        top, bottom = add_arrived(q, 3, SLOTS)
        cols = pl.ds(q * CHUNK, CHUNK)
        y_ref[0:hr, cols] = top.astype(y_ref.dtype)
        y_ref[hr:s, cols] = bottom.astype(y_ref.dtype)

    def prologue():
        gates_out()
        for e in range(el):
            w1_own(e).wait()
            w1_copy(2, e).wait_recv()
        x_own.wait()
        hiddens(0, 1, 0, el, 0, 1)

    def first_halves():
        cx_copy(0).wait_recv()
        cx_copy(2).wait_recv()
        cx_copy(4).start()
        cx_copy(5).start()

    def seconds():
        cx_copy(1).wait_recv()
        cx_copy(3).wait_recv()

    def opposite():
        cx_copy(4).wait_recv()
        cx_copy(5).wait_recv()

    def chunk(q, step):
        if step == 0:
            loaded(q)
        hop(q, step)

    seen = set()

    def need(*key):
        if key not in seen:
            seen.add(key)
            arrived(w1_copy, key[:2], key[2])

    def units(b0, n, e0, e1, far_slice):
        if b0:
            once(seconds)
        if b0 == 3:
            once(opposite)
        for e in range(e0, e1):
            need(*((7, 8) if far_slice else (5, 6)), e)
        hiddens(b0, n, e0, e1, *((3, 4) if far_slice else (0 if b0 else 1, 3)))

    def once(fn):
        if fn not in seen:
            seen.add(fn)
            fn()

    run = {
        "N1": lambda e: near(w1_copy, e), "F1": lambda e: far(w1_copy, e),
        "X1": first_halves, "X2": lambda: once(seconds), "X3": lambda: once(opposite),
        "G": gates_in, "H": units,
        "W": lambda q: start(w2_copy, (0, 1, 2), q),
        "N2": lambda q: near(w2_copy, q), "F2": lambda q: far(w2_copy, q), "L": load,
        "R": chunk, "E": finish,
    }
    prologue()
    for op, *args in PROGRAM:
        run[op](*args)

    for copies in sent[-SLOTS:]:
        for copy in copies:
            copy.wait_send()
    for kind in range(6):
        cx_copy(kind).wait_send()
    for kind in range(3):
        g_copy(kind).wait_send()
    for kind in range(9):
        for q in range(nq):
            w2_copy(kind, q).wait_send()


def solution(mesh):
    ntp = mesh.shape["tp"]
    nep = mesh.shape["ep"]
    nx = nep // CORES

    def body(x, idx, gates, w1, w2):
        t_n, h = x.shape
        el, fs = w1.shape[0], w1.shape[2]
        n_exp = el * nep
        k = idx.shape[1]
        s = t_n // ntp
        cap = 8 * ((5 * k * s + 32 * n_exp - 1) // (32 * n_exp))
        kb = ntp * fs
        nb = h // kb
        nq = h // CHUNK
        rows = -(-CORES * el // 8) * 8
        bf16, f32, dma = jnp.bfloat16, jnp.float32, pltpu.SemaphoreType.DMA
        any_space = pl.BlockSpec(memory_space=pl.ANY)
        y, _ = pl.pallas_call(
            functools.partial(kernel, ntp=ntp, nep=nep, cap=cap),
            out_shape=(jax.ShapeDtypeStruct((s, h), bf16),
                       jax.ShapeDtypeStruct(((nq - DIRECT) * CORES * el, kb, CHUNK), bf16)),
            in_specs=[any_space] * 5,
            out_specs=(pl.BlockSpec(memory_space=pltpu.VMEM), any_space),
            scratch_shapes=[
                pltpu.VMEM((4, s, h), bf16),
                pltpu.VMEM((k, s), jnp.int32),
                pltpu.VMEM((k, s), f32),
                pltpu.VMEM((nx, rows, s), f32),
                pltpu.VMEM((4, rows, s), f32),
                pltpu.VMEM((4, s, 128), f32),
                pltpu.VMEM((nq * CORES * el, kb, CHUNK), bf16),
                pltpu.VMEM((DIRECT * CORES * el, kb, CHUNK), bf16),
                pltpu.VMEM((4 * CORES * el, s, kb), bf16),
                pltpu.VMEM((2, nq, 3, s // 2, CHUNK), f32),
                pltpu.VMEM((SLOTS + 1, s, CHUNK), f32),
                dma((3,)), dma((6,)), dma((6,)), dma((3,)), dma((3,)), dma((el,)),
                dma((9, el)), dma((9, el)), dma((9, nq)), dma((9, nq)),
                dma((3, nq)), dma((2, nq, 3)), dma((2, nq, 3)),
            ],
            compiler_params=pltpu.CompilerParams(
                collective_id=0, has_side_effects=True, vmem_limit_bytes=67_000_000),
        )(x, idx.T, gates.T, w1.reshape(el, nb, kb, fs), w2)
        return y

    row = P(("dp", "ep"), None)
    return jax.shard_map(
        body,
        mesh=mesh,
        in_specs=(row, row, row, P("ep", None, "tp"), P("ep", "tp", None)),
        out_specs=P(("dp", "ep", "tp"), None),
        check_vma=False,
    )
```

```python
import functools

import jax
import jax.numpy as jnp
from jax import lax
from jax.experimental import pallas as pl
from jax.experimental.pallas import tpu as pltpu
from jax.sharding import PartitionSpec as P


MESH = pl.DeviceIdType.MESH
CORES = 2
CHUNK = 256
SLOTS = 6
DIRECT = 2
CHUNKS = ((0, 0, 128), (0, 128, 128), (1, 0, 256), (2, 0, 256), (3, 0, 256), (4, 0, 256), (5, 0, 256))
RING = ((1, 2), (3, 3), (2, 1), (0, 0))
PROGRAM = (
    ("N1", 1), ("X1",), ("G",), ("W", 1), ("N1", 0), ("N1", 2), ("H", 0, 1, 0, 2, 0), ("N1", 3),
    ("H", 1, 2, 0, 3, 0), ("N1", 4), ("F1", 1), ("H", 1, 2, 3, 5, 0), ("H", 0, 1, 2, 5, 0),
    ("N2", 1), ("W", 0), ("F1", 0), ("W", 2), ("H", 3, 1, 2, 5, 0), ("F1", 3), ("F1", 2),
    ("H", 3, 1, 0, 2, 0), ("H", 1, 2, 2, 4, 1), ("F2", 1), ("F1", 4), ("H", 1, 2, 0, 2, 1),
    ("L", 1), ("H", 1, 2, 4, 5, 1), ("C", 1, 0), ("N2", 0), ("S", 1, 0), ("H", 3, 1, 0, 5, 1),
    ("C", 1, 1), ("N2", 2), ("S", 1, 1), ("F2", 0), ("W", 3), ("W", 6), ("L", 0), ("C", 0, 0),
    ("S", 0, 0), ("X2",), ("C", 1, 2), ("F2", 2), ("S", 1, 2), ("L", 2), ("C", 2, 0), ("S", 2, 0),
    ("H", 0, 1, 0, 5, 1), ("C", 0, 1), ("S", 0, 1), ("C", 2, 1), ("N2", 3), ("C", 0, 2),
    ("S", 2, 1), ("N2", 6), ("S", 0, 2), ("W", 4), ("C", 2, 2), ("F2", 3), ("L", 3), ("F2", 6),
    ("S", 2, 2), ("L", 6), ("C", 3, 0), ("S", 3, 0), ("C", 0, 3), ("C", 6, 0), ("X3",), ("W", 5),
    ("S", 6, 0), ("C", 6, 1), ("N2", 4), ("C", 3, 1), ("S", 0, 3), ("S", 3, 1), ("C", 2, 3),
    ("C", 6, 2), ("F2", 4), ("S", 6, 1), ("C", 3, 2), ("S", 3, 2), ("C", 3, 3), ("L", 4), ("N2", 5),
    ("S", 6, 2), ("F2", 5), ("L", 5), ("C", 4, 0), ("S", 4, 0), ("C", 5, 0), ("S", 5, 0),
    ("C", 4, 1), ("S", 4, 1), ("C", 5, 1), ("C", 6, 3), ("S", 6, 3), ("S", 2, 3), ("C", 4, 3),
    ("S", 5, 1), ("C", 1, 3), ("C", 5, 2), ("C", 4, 2), ("S", 4, 2), ("C", 5, 3), ("S", 1, 3),
    ("S", 5, 2), ("S", 3, 3), ("S", 4, 3), ("S", 5, 3),
)


def kernel(x_ref, idx_ref, gates_ref, w1_ref, w2_ref, y_ref, w2f, xb, ids, gs, gto, gtb, gb, wb, wv,
           ab, rb, part, xl_sem, x_snd, x_rcv, g_snd, g_rcv, l1_sem, w1_snd, w1_rcv, w2_snd, w2_rcv,
           ld_sem, rs_snd, rs_rcv, *, ntp, nep, cap):
    s, h = xb.shape[1:]
    el, nb = w1_ref.shape[0], w1_ref.shape[1]
    fs = w1_ref.shape[3]
    kb = ntp * fs
    hr = s // 2
    nq = h // CHUNK
    nx = nep // CORES

    ep, y = lax.axis_index("ep"), lax.axis_index("tp")
    core, cx = lax.rem(ep, CORES), lax.div(ep, CORES)

    def along_x(d):
        return {"ep": lax.rem(cx + d, nx) * CORES + core}

    right, left, across = along_x(1), along_x(nx - 1), along_x(2)
    up, down = {"tp": lax.rem(y + 1, ntp)}, {"tp": lax.rem(y + ntp - 1, ntp)}
    peer = {"ep": cx * CORES + (CORES - 1 - core)}

    barrier = pltpu.get_barrier_semaphore()
    for dev in (right, left, across, up, down, peer):
        pl.semaphore_signal(barrier, inc=1, device_id=dev, device_id_type=MESH)
    pl.semaphore_wait(barrier, 6)

    def remote(src, dst, snd, rcv, dev):
        return pltpu.make_async_remote_copy(
            src_ref=src, dst_ref=dst, send_sem=snd, recv_sem=rcv, device_id=dev,
            device_id_type=MESH)

    x0 = pl.multiple_of(y * s, s)
    lo, hi = pl.ds(0, hr), pl.ds(hr, hr)

    def cx_copy(kind):
        src = (x_ref.at[pl.ds(x0, hr)], x_ref.at[pl.ds(x0 + hr, hr)], x_ref.at[pl.ds(x0 + hr, hr)],
               x_ref.at[pl.ds(x0, hr)], xb.at[1, lo], xb.at[2, hi])[kind]
        dst = (xb.at[1, lo], xb.at[1, hi], xb.at[2, hi], xb.at[2, lo], xb.at[3, lo], xb.at[3, hi])[kind]
        dev = (right, right, left, left, right, left)[kind]
        return remote(src, dst, x_snd.at[kind], x_rcv.at[kind], dev)

    def g_copy(kind):
        far, slot, dev = ((1, 1, right), (3, 2, left), (2, 3, across))[kind]
        return remote(gto.at[far], gtb.at[slot], g_snd.at[kind], g_rcv.at[kind], dev)

    h1 = wb.shape[1] // 2
    mine, others = pl.ds(0, fs), pl.ds(fs, fs)
    whole1, a1, b1 = pl.ds(0, 2 * h1), pl.ds(0, h1), pl.ds(h1, h1)

    def w1_copy(kind, e):
        def at(slot, rows, lanes):
            return wb.at[pl.ds((e * ntp + slot) * nb, nb), rows, lanes]

        src, dst, dev = (
            lambda: (w1_ref.at[e], at(1, whole1, mine), up),
            lambda: (w1_ref.at[e], at(2, whole1, mine), down),
            lambda: (w1_ref.at[e], at(0, whole1, others), peer),
            lambda: (at(1, a1, mine), at(3, a1, mine), up),
            lambda: (at(2, b1, mine), at(3, b1, mine), down),
            lambda: (at(1, whole1, mine), at(1, whole1, others), peer),
            lambda: (at(2, whole1, mine), at(2, whole1, others), peer),
            lambda: (at(3, a1, mine), at(3, a1, others), peer),
            lambda: (at(3, b1, mine), at(3, b1, others), peer),
        )[kind]()
        return remote(src, dst, w1_snd.at[kind, e], w1_rcv.at[kind, e], dev)

    def w2_copy(kind, i):
        q, lane0, width = CHUNKS[i]

        def at(slot, off, n, cs):
            buf, at_q = (wv, q) if q < DIRECT else (w2f, q - DIRECT)
            return buf.at[pl.ds((at_q * CORES + cs) * el, el), pl.ds(slot * fs + off, n),
                          pl.ds(lane0, width)]

        own = w2_ref.at[:, :, pl.ds(q * CHUNK + lane0, width)]
        hf = fs // 2
        src, dst, dev = (
            lambda: (own, at(1, 0, fs, 0), up),
            lambda: (own, at(2, 0, fs, 0), down),
            lambda: (own, at(0, 0, fs, 1), peer),
            lambda: (at(1, 0, hf, 0), at(3, 0, hf, 0), up),
            lambda: (at(2, hf, hf, 0), at(3, hf, hf, 0), down),
            lambda: (at(1, 0, fs, 0), at(1, 0, fs, 1), peer),
            lambda: (at(2, 0, fs, 0), at(2, 0, fs, 1), peer),
            lambda: (at(3, 0, hf, 0), at(3, 0, hf, 1), peer),
            lambda: (at(3, hf, hf, 0), at(3, hf, hf, 1), peer),
        )[kind]()
        return remote(src, dst, w2_snd.at[kind, i], w2_rcv.at[kind, i], dev)

    def start(copy, kinds, n):
        for kind in kinds:
            copy(kind, n).start()

    def arrived(copy, kinds, n):
        for kind in kinds:
            copy(kind, n).wait_recv()

    def near(copy, n):
        arrived(copy, (0, 1), n)
        start(copy, (3, 4, 5, 6), n)

    def far(copy, n):
        arrived(copy, (3, 4), n)
        start(copy, (7, 8), n)

    x_own = pltpu.make_async_copy(x_ref.at[pl.ds(x0, s)], xb.at[0], xl_sem.at[0])
    tokens = pl.ds(x0, s)
    idx_own = pltpu.make_async_copy(idx_ref.at[:, tokens], ids, xl_sem.at[1])
    gates_own = pltpu.make_async_copy(gates_ref.at[:, tokens], gs, xl_sem.at[2])

    def w2_own(q):
        return pltpu.make_async_copy(
            w2_ref.at[:, :, pl.ds(q * CHUNK, CHUNK)],
            wv.at[pl.ds(q * CORES * el, el), pl.ds(0, fs), :], ld_sem.at[0, q])

    def w1_own(e):
        return pltpu.make_async_copy(
            w1_ref.at[e], wb.at[pl.ds(e * ntp * nb, nb), :, mine], l1_sem.at[e])

    idx_own.start()
    gates_own.start()
    start(w1_copy, (0, 1, 2), 0)
    for kind in range(4):
        cx_copy(kind).start()
    x_own.start()
    w1_own(0).start()
    for e in range(1, el):
        start(w1_copy, (0, 1, 2), e)
        w1_own(e).start()
    for q in range(DIRECT):
        w2_own(q).start()

    def gates_out():
        idx_own.wait()
        gates_own.wait()
        v = ids[...]
        block = jnp.zeros(v.shape, jnp.int32)
        for m in range(1, nep):
            block = block + (v >= el * m).astype(jnp.int32)
        swap = jnp.where((block & 1) == core, 0, el)
        n = gto.shape[1]
        row = (((block >> 1) - cx + nx) & (nx - 1)) * n + swap + (v - el * block)
        rows = lax.broadcasted_iota(jnp.int32, (nx * n, s), 0)
        one = jnp.zeros((nx * n, s), jnp.float32)
        dense = jnp.zeros((nx * n, s), jnp.float32)
        for k in range(v.shape[0]):
            hit = rows == row[k:k + 1]
            one = one + jnp.where(hit, 1.0, 0.0)
            dense = dense + jnp.where(hit, gs[k:k + 1], 0.0)
        before = (lax.broadcasted_iota(jnp.int32, (s, s), 0)
                  < lax.broadcasted_iota(jnp.int32, (s, s), 1))
        slot = jnp.dot(one.astype(jnp.bfloat16), jnp.where(before, 1.0, 0.0).astype(jnp.bfloat16),
                       preferred_element_type=jnp.float32)
        kept = jnp.where(slot < cap, dense, 0.0).reshape(nx, n, s)
        gto[...] = kept
        gtb[0] = kept[0]
        for kind in range(3):
            g_copy(kind).start()

    def gates_in():
        for kind in range(3):
            g_copy(kind).wait_recv()
        for b in range(4):
            g = gtb[b]
            pad = jnp.zeros((128 - g.shape[0], s), jnp.float32)
            gb[b] = jnp.transpose(jnp.concatenate([g, pad], axis=0))

    def hidden(b0, n, e, slot):
        w = wb[pl.ds((e * ntp + slot) * nb, nb)].reshape(h, CORES * fs)
        z = jnp.dot(xb[b0:b0 + n].reshape(n * s, h), w, preferred_element_type=jnp.float32)
        t = jnp.tanh(z * (0.7978845608028654 + 0.035677408136300125 * (z * z)))
        a = ((0.5 * z) * (1.0 + t)).astype(jnp.bfloat16)
        cols = pl.ds(pl.multiple_of(slot * fs, fs), fs)
        for b in range(n):
            rows = a[b * s:(b + 1) * s]
            for cs in range(CORES):
                ab[(b0 + b) * CORES * el + cs * el + e, :, cols] = rows[:, cs * fs:(cs + 1) * fs]

    def hiddens(b0, n, e0, e1, s0, s1):
        def step(i, _):
            hidden(b0, n, e0 + lax.div(i, s1 - s0), s0 + lax.rem(i, s1 - s0))
            return 0
        lax.fori_loop(0, (e1 - e0) * (s1 - s0), step, 0)

    def loads(q):
        src, dst = (q - DIRECT) * CORES * el, (q - DIRECT) * CORES * el
        return (
            pltpu.make_async_copy(w2_ref.at[:, :, pl.ds(q * CHUNK, CHUNK)],
                                  wb.at[pl.ds(dst, el), pl.ds(0, fs), :], ld_sem.at[0, q]),
            pltpu.make_async_copy(w2f.at[pl.ds(src, el), pl.ds(fs, kb - fs), :],
                                  wb.at[pl.ds(dst, el), pl.ds(fs, kb - fs), :], ld_sem.at[1, q]),
            pltpu.make_async_copy(w2f.at[pl.ds(src + el, el)], wb.at[pl.ds(dst + el, el)],
                                  ld_sem.at[2, q]),
        )

    def w1_sent():
        for kind in range(9):
            for e in range(el):
                w1_copy(kind, e).wait_send()

    def load(i):
        arrived(w2_copy, (2, 5, 6, 7, 8), i)
        q = CHUNKS[i][0]
        if q < DIRECT:
            if ("own", q) not in seen:
                seen.add(("own", q))
                w2_own(q).wait()
            return
        once(w1_sent)
        for copy in loads(q):
            copy.start()

    lane = lax.broadcasted_iota(jnp.int32, (s, 128), 1)

    def halves(ref, r, l, off):
        if r == l:
            return ref[r * off[0] + off[1]]
        return jnp.concatenate(
            [ref[r * off[0] + off[1], 0:hr], ref[l * off[0] + off[1], hr:s]], axis=0)

    loaded = set()
    slots = {}
    sent = []

    def outputs(i, step):
        q, lane0, width = CHUNKS[i]
        if q >= DIRECT and q not in loaded:
            loaded.add(q)
            for copy in loads(q):
                copy.wait()
        if len(slots) < SLOTS:
            k = min(set(range(SLOTS)) - set(slots.values()))
        else:
            old = next(key for key in sent if key in slots)
            k = slots.pop(old)
            for copy in ring(*old, k):
                copy.wait_send()
        slots[i, step] = k
        r, l = RING[step]
        lanes = pl.ds(lane0, width)
        mine = pl.ds(0, width)

        def gated(e, cs):
            n = cs * el + e
            w = (wv.at[q * CORES * el + n, :, lanes] if q < DIRECT
                 else wb.at[(q - DIRECT) * CORES * el + n, :, lanes])
            o = jnp.dot(halves(ab, r, l, (CORES * el, n)), w[...], preferred_element_type=jnp.float32)
            o = o.astype(jnp.bfloat16).astype(jnp.float32)
            col = jnp.sum(jnp.where(lane == n, halves(gb, r, l, (1, 0)), 0.0), axis=1, keepdims=True)
            return jnp.where(col != 0.0, o * col, 0.0)

        part[k, :, mine] = jnp.zeros((s, width), jnp.float32)

        def more(e, _):
            part[k, :, mine] = part[k, :, mine] + (gated(e, 0) + gated(e, 1))
            return 0
        lax.fori_loop(0, el, more, 0)

    def ring(i, step, k):
        q, lane0, width = CHUNKS[i]
        lanes = pl.ds(lane0, width)
        return tuple(
            remote(part.at[k, rows, pl.ds(0, width)], rb.at[d, q, step, :, lanes],
                   rs_snd.at[d, i, step], rs_rcv.at[d, i, step], dev)
            for d, rows, dev in ((0, lo, right), (1, hi, left)))

    def hop(i, step):
        q, lane0, width = CHUNKS[i]
        lanes = pl.ds(lane0, width)
        k = slots[i, step]
        for d, copy in enumerate(ring(i, step - 1, k) if step else ()):
            copy.wait_recv()
        for d, first in ((0, 0), (1, hr)):
            rows = pl.ds(first, hr)
            if step == 3:
                y_ref[rows, pl.ds(q * CHUNK + lane0, width)] = (
                    part[k, rows, 0:width] + rb[d, q, 2, :, lanes]).astype(y_ref.dtype)
            elif step:
                part[k, rows, 0:width] = part[k, rows, 0:width] + rb[d, q, step - 1, :, lanes]
        if step == 3:
            del slots[i, step]
        else:
            for copy in ring(i, step, k):
                copy.start()
            sent.append((i, step))

    def prologue():
        gates_out()
        for e in range(el):
            w1_own(e).wait()
            w1_copy(2, e).wait_recv()
        x_own.wait()
        hiddens(0, 1, 0, el, 0, 1)

    def first_halves():
        cx_copy(0).wait_recv()
        cx_copy(2).wait_recv()
        cx_copy(4).start()
        cx_copy(5).start()

    def seconds():
        cx_copy(1).wait_recv()
        cx_copy(3).wait_recv()

    def opposite():
        cx_copy(4).wait_recv()
        cx_copy(5).wait_recv()

    seen = set()

    def need(*key):
        if key not in seen:
            seen.add(key)
            arrived(w1_copy, key[:2], key[2])

    def units(b0, n, e0, e1, far_slice):
        if b0:
            once(seconds)
        if b0 == 3:
            once(opposite)
        for e in range(e0, e1):
            need(*((7, 8) if far_slice else (5, 6)), e)
        hiddens(b0, n, e0, e1, *((3, 4) if far_slice else (0 if b0 else 1, 3)))

    def once(fn):
        if fn not in seen:
            seen.add(fn)
            fn()

    run = {
        "N1": lambda e: near(w1_copy, e), "F1": lambda e: far(w1_copy, e),
        "X1": first_halves, "X2": lambda: once(seconds), "X3": lambda: once(opposite),
        "G": gates_in, "H": units,
        "W": lambda q: start(w2_copy, (0, 1, 2), q),
        "N2": lambda q: near(w2_copy, q), "F2": lambda q: far(w2_copy, q), "L": load,
        "C": outputs, "S": hop,
    }
    prologue()
    for op, *args in PROGRAM:
        run[op](*args)

    for key in sent:
        if key in slots:
            for copy in ring(*key, slots[key]):
                copy.wait_send()
    for kind in range(6):
        cx_copy(kind).wait_send()
    for kind in range(3):
        g_copy(kind).wait_send()
    for kind in range(9):
        for i in range(len(CHUNKS)):
            w2_copy(kind, i).wait_send()


def solution(mesh):
    ntp = mesh.shape["tp"]
    nep = mesh.shape["ep"]
    nx = nep // CORES

    def body(x, idx, gates, w1, w2):
        t_n, h = x.shape
        el, fs = w1.shape[0], w1.shape[2]
        n_exp = el * nep
        k = idx.shape[1]
        s = t_n // ntp
        cap = 8 * ((5 * k * s + 32 * n_exp - 1) // (32 * n_exp))
        kb = ntp * fs
        nb = h // kb
        nq = h // CHUNK
        rows = -(-CORES * el // 8) * 8
        bf16, f32, dma = jnp.bfloat16, jnp.float32, pltpu.SemaphoreType.DMA
        any_space = pl.BlockSpec(memory_space=pl.ANY)
        y, _ = pl.pallas_call(
            functools.partial(kernel, ntp=ntp, nep=nep, cap=cap),
            out_shape=(jax.ShapeDtypeStruct((s, h), bf16),
                       jax.ShapeDtypeStruct(((nq - DIRECT) * CORES * el, kb, CHUNK), bf16)),
            in_specs=[any_space] * 5,
            out_specs=(pl.BlockSpec(memory_space=pltpu.VMEM), any_space),
            scratch_shapes=[
                pltpu.VMEM((4, s, h), bf16),
                pltpu.VMEM((k, s), jnp.int32),
                pltpu.VMEM((k, s), f32),
                pltpu.VMEM((nx, rows, s), f32),
                pltpu.VMEM((4, rows, s), f32),
                pltpu.VMEM((4, s, 128), f32),
                pltpu.VMEM((nq * CORES * el, kb, CHUNK), bf16),
                pltpu.VMEM((DIRECT * CORES * el, kb, CHUNK), bf16),
                pltpu.VMEM((4 * CORES * el, s, kb), bf16),
                pltpu.VMEM((2, nq, 3, s // 2, CHUNK), f32),
                pltpu.VMEM((SLOTS, s, CHUNK), f32),
                dma((3,)), dma((6,)), dma((6,)), dma((3,)), dma((3,)), dma((el,)),
                dma((9, el)), dma((9, el)), dma((9, len(CHUNKS))), dma((9, len(CHUNKS))),
                dma((3, nq)), dma((2, len(CHUNKS), 3)), dma((2, len(CHUNKS), 3)),
            ],
            compiler_params=pltpu.CompilerParams(
                collective_id=0, has_side_effects=True, vmem_limit_bytes=67_000_000),
        )(x, idx.T, gates.T, w1.reshape(el, nb, kb, fs), w2)
        return y

    row = P(("dp", "ep"), None)
    return jax.shard_map(
        body,
        mesh=mesh,
        in_specs=(row, row, row, P("ep", None, "tp"), P("ep", "tp", None)),
        out_specs=P(("dp", "ep", "tp"), None),
        check_vma=False,
    )
```

```python
import functools

import jax
import jax.numpy as jnp
from jax import lax
from jax.experimental import pallas as pl
from jax.experimental.pallas import tpu as pltpu
from jax.sharding import PartitionSpec as P


MESH = pl.DeviceIdType.MESH
CORES = 2
CHUNK = 256
SLOTS = 5
DIRECT = 2
RING = ((1, 2), (3, 3), (2, 1), (0, 0))
PROGRAM = (
    ("N1", 0), ("X1",), ("N1", 1), ("W", 0), ("N1", 2), ("H", 0, 1, 0, 2, 0), ("H", 1, 2, 0, 3, 0),
    ("N1", 3), ("N1", 4), ("F1", 0), ("H", 1, 2, 3, 5, 0), ("H", 3, 1, 2, 5, 0), ("N2", 0),
    ("F1", 1), ("H", 3, 1, 0, 2, 0), ("H", 1, 2, 0, 2, 1), ("F1", 2), ("W", 1),
    ("H", 0, 1, 2, 5, 0), ("F1", 3), ("F1", 4), ("X2",), ("H", 1, 2, 2, 4, 1), ("F2", 0), ("G",),
    ("H", 1, 2, 4, 5, 1), ("L", 0), ("X3",), ("R", 0, 0), ("N2", 1), ("H", 3, 1, 0, 5, 1), ("W", 2),
    ("R", 0, 1), ("F2", 1), ("L", 1), ("R", 1, 0), ("H", 0, 1, 0, 5, 1), ("N2", 2), ("R", 0, 2),
    ("W", 3), ("F2", 2), ("R", 1, 1), ("W", 5), ("L", 2), ("R", 2, 0), ("E", 0), ("N2", 3),
    ("R", 1, 2), ("W", 4), ("R", 2, 1), ("F2", 3), ("L", 3), ("R", 3, 0), ("R", 2, 2), ("N2", 4),
    ("F2", 4), ("R", 3, 1), ("L", 4), ("N2", 5), ("E", 2), ("R", 4, 0), ("R", 3, 2), ("F2", 5),
    ("L", 5), ("E", 1), ("R", 5, 0), ("E", 3), ("R", 4, 1), ("R", 5, 1), ("R", 4, 2), ("R", 5, 2),
    ("E", 4), ("E", 5),
)


def kernel(x_ref, idx_ref, gates_ref, w1_ref, w2_ref, y_ref, w2f, xb, ids, gs, gto, gtb, gb, wb, wv,
           ab, rb, part, xl_sem, x_snd, x_rcv, g_snd, g_rcv, l1_sem, w1_snd, w1_rcv, w2_snd, w2_rcv,
           ld_sem, rs_snd, rs_rcv, *, ntp, nep, cap):
    s, h = xb.shape[1:]
    el, nb = w1_ref.shape[0], w1_ref.shape[1]
    fs = w1_ref.shape[3]
    kb = ntp * fs
    hr = s // 2
    nq = h // CHUNK
    nx = nep // CORES

    ep, y = lax.axis_index("ep"), lax.axis_index("tp")
    core, cx = lax.rem(ep, CORES), lax.div(ep, CORES)

    def along_x(d):
        return {"ep": lax.rem(cx + d, nx) * CORES + core}

    right, left, across = along_x(1), along_x(nx - 1), along_x(2)
    up, down = {"tp": lax.rem(y + 1, ntp)}, {"tp": lax.rem(y + ntp - 1, ntp)}
    peer = {"ep": cx * CORES + (CORES - 1 - core)}

    barrier = pltpu.get_barrier_semaphore()
    for dev in (right, left, across, up, down, peer):
        pl.semaphore_signal(barrier, inc=1, device_id=dev, device_id_type=MESH)
    pl.semaphore_wait(barrier, 6)

    def remote(src, dst, snd, rcv, dev):
        return pltpu.make_async_remote_copy(
            src_ref=src, dst_ref=dst, send_sem=snd, recv_sem=rcv, device_id=dev,
            device_id_type=MESH)

    x0 = pl.multiple_of(y * s, s)
    lo, hi = pl.ds(0, hr), pl.ds(hr, hr)

    def cx_copy(kind):
        src = (x_ref.at[pl.ds(x0, hr)], x_ref.at[pl.ds(x0 + hr, hr)], x_ref.at[pl.ds(x0 + hr, hr)],
               x_ref.at[pl.ds(x0, hr)], xb.at[1, lo], xb.at[2, hi])[kind]
        dst = (xb.at[1, lo], xb.at[1, hi], xb.at[2, hi], xb.at[2, lo], xb.at[3, lo], xb.at[3, hi])[kind]
        dev = (right, right, left, left, right, left)[kind]
        return remote(src, dst, x_snd.at[kind], x_rcv.at[kind], dev)

    def g_copy(kind):
        far, slot, dev = ((1, 1, right), (3, 2, left), (2, 3, across))[kind]
        return remote(gto.at[far], gtb.at[slot], g_snd.at[kind], g_rcv.at[kind], dev)

    h1 = wb.shape[1] // 2
    mine, others = pl.ds(0, fs), pl.ds(fs, fs)
    whole1, a1, b1 = pl.ds(0, 2 * h1), pl.ds(0, h1), pl.ds(h1, h1)

    def w1_copy(kind, e):
        def at(slot, rows, lanes):
            return wb.at[pl.ds((e * ntp + slot) * nb, nb), rows, lanes]

        src, dst, dev = (
            lambda: (w1_ref.at[e], at(1, whole1, mine), up),
            lambda: (w1_ref.at[e], at(2, whole1, mine), down),
            lambda: (w1_ref.at[e], at(0, whole1, others), peer),
            lambda: (at(1, a1, mine), at(3, a1, mine), up),
            lambda: (at(2, b1, mine), at(3, b1, mine), down),
            lambda: (at(1, whole1, mine), at(1, whole1, others), peer),
            lambda: (at(2, whole1, mine), at(2, whole1, others), peer),
            lambda: (at(3, a1, mine), at(3, a1, others), peer),
            lambda: (at(3, b1, mine), at(3, b1, others), peer),
        )[kind]()
        return remote(src, dst, w1_snd.at[kind, e], w1_rcv.at[kind, e], dev)

    def w2_copy(kind, q):
        def at(slot, off, n, cs):
            buf, at_q = (wv, q) if q < DIRECT else (w2f, q - DIRECT)
            return buf.at[pl.ds((at_q * CORES + cs) * el, el), pl.ds(slot * fs + off, n), :]

        own = w2_ref.at[:, :, pl.ds(q * CHUNK, CHUNK)]
        hf = fs // 2
        src, dst, dev = (
            lambda: (own, at(1, 0, fs, 0), up),
            lambda: (own, at(2, 0, fs, 0), down),
            lambda: (own, at(0, 0, fs, 1), peer),
            lambda: (at(1, 0, hf, 0), at(3, 0, hf, 0), up),
            lambda: (at(2, hf, hf, 0), at(3, hf, hf, 0), down),
            lambda: (at(1, 0, fs, 0), at(1, 0, fs, 1), peer),
            lambda: (at(2, 0, fs, 0), at(2, 0, fs, 1), peer),
            lambda: (at(3, 0, hf, 0), at(3, 0, hf, 1), peer),
            lambda: (at(3, hf, hf, 0), at(3, hf, hf, 1), peer),
        )[kind]()
        return remote(src, dst, w2_snd.at[kind, q], w2_rcv.at[kind, q], dev)

    def start(copy, kinds, n):
        for kind in kinds:
            copy(kind, n).start()

    def arrived(copy, kinds, n):
        for kind in kinds:
            copy(kind, n).wait_recv()

    def near(copy, n):
        arrived(copy, (0, 1), n)
        start(copy, (3, 4, 5, 6), n)

    def far(copy, n):
        arrived(copy, (3, 4), n)
        start(copy, (7, 8), n)

    x_own = pltpu.make_async_copy(x_ref.at[pl.ds(x0, s)], xb.at[0], xl_sem.at[0])
    tokens = pl.ds(x0, s)
    idx_own = pltpu.make_async_copy(idx_ref.at[:, tokens], ids, xl_sem.at[1])
    gates_own = pltpu.make_async_copy(gates_ref.at[:, tokens], gs, xl_sem.at[2])

    def w2_own(q):
        return pltpu.make_async_copy(
            w2_ref.at[:, :, pl.ds(q * CHUNK, CHUNK)],
            wv.at[pl.ds(q * CORES * el, el), pl.ds(0, fs), :], ld_sem.at[0, q])

    def w1_own(e):
        return pltpu.make_async_copy(
            w1_ref.at[e], wb.at[pl.ds(e * ntp * nb, nb), :, mine], l1_sem.at[e])

    idx_own.start()
    gates_own.start()
    start(w1_copy, (0, 1, 2), 0)
    for kind in range(4):
        cx_copy(kind).start()
    x_own.start()
    w1_own(0).start()
    for e in range(1, el):
        start(w1_copy, (0, 1, 2), e)
        w1_own(e).start()
    for q in range(DIRECT):
        w2_own(q).start()

    def gates_out():
        idx_own.wait()
        gates_own.wait()
        v = ids[...]
        block = jnp.zeros(v.shape, jnp.int32)
        for m in range(1, nep):
            block = block + (v >= el * m).astype(jnp.int32)
        swap = jnp.where((block & 1) == core, 0, el)
        n = gto.shape[1]
        row = (((block >> 1) - cx + nx) & (nx - 1)) * n + swap + (v - el * block)
        rows = lax.broadcasted_iota(jnp.int32, (nx * n, s), 0)
        one = jnp.zeros((nx * n, s), jnp.float32)
        dense = jnp.zeros((nx * n, s), jnp.float32)
        for k in range(v.shape[0]):
            hit = rows == row[k:k + 1]
            one = one + jnp.where(hit, 1.0, 0.0)
            dense = dense + jnp.where(hit, gs[k:k + 1], 0.0)
        before = (lax.broadcasted_iota(jnp.int32, (s, s), 0)
                  < lax.broadcasted_iota(jnp.int32, (s, s), 1))
        slot = jnp.dot(one.astype(jnp.bfloat16), jnp.where(before, 1.0, 0.0).astype(jnp.bfloat16),
                       preferred_element_type=jnp.float32)
        kept = jnp.where(slot < cap, dense, 0.0).reshape(nx, n, s)
        gto[...] = kept
        gtb[0] = kept[0]
        for kind in range(3):
            g_copy(kind).start()

    def gates_in():
        for kind in range(3):
            g_copy(kind).wait_recv()
        for b in range(4):
            g = gtb[b]
            pad = jnp.zeros((128 - g.shape[0], s), jnp.float32)
            gb[b] = jnp.transpose(jnp.concatenate([g, pad], axis=0))

    def hidden(b0, n, e, slot):
        w = wb[pl.ds((e * ntp + slot) * nb, nb)].reshape(h, CORES * fs)
        z = jnp.dot(xb[b0:b0 + n].reshape(n * s, h), w, preferred_element_type=jnp.float32)
        t = jnp.tanh(z * (0.7978845608028654 + 0.035677408136300125 * (z * z)))
        a = ((0.5 * z) * (1.0 + t)).astype(jnp.bfloat16)
        cols = pl.ds(pl.multiple_of(slot * fs, fs), fs)
        for b in range(n):
            rows = a[b * s:(b + 1) * s]
            for cs in range(CORES):
                ab[(b0 + b) * CORES * el + cs * el + e, :, cols] = rows[:, cs * fs:(cs + 1) * fs]

    def hiddens(b0, n, e0, e1, s0, s1):
        def step(i, _):
            hidden(b0, n, e0 + lax.div(i, s1 - s0), s0 + lax.rem(i, s1 - s0))
            return 0
        lax.fori_loop(0, (e1 - e0) * (s1 - s0), step, 0)

    def loads(q):
        src, dst = (q - DIRECT) * CORES * el, (q - DIRECT) * CORES * el
        return (
            pltpu.make_async_copy(w2_ref.at[:, :, pl.ds(q * CHUNK, CHUNK)],
                                  wb.at[pl.ds(dst, el), pl.ds(0, fs), :], ld_sem.at[0, q]),
            pltpu.make_async_copy(w2f.at[pl.ds(src, el), pl.ds(fs, kb - fs), :],
                                  wb.at[pl.ds(dst, el), pl.ds(fs, kb - fs), :], ld_sem.at[1, q]),
            pltpu.make_async_copy(w2f.at[pl.ds(src + el, el)], wb.at[pl.ds(dst + el, el)],
                                  ld_sem.at[2, q]),
        )

    def w1_sent():
        for kind in range(9):
            for e in range(el):
                w1_copy(kind, e).wait_send()

    def load(q):
        arrived(w2_copy, (2, 5, 6, 7, 8), q)
        if q < DIRECT:
            w2_own(q).wait()
            return
        once(w1_sent)
        for copy in loads(q):
            copy.start()

    def loaded(q):
        if q >= DIRECT:
            for copy in loads(q):
                copy.wait()

    lane = lax.broadcasted_iota(jnp.int32, (s, 128), 1)

    def halves(ref, r, l, off):
        if r == l:
            return ref[r * off[0] + off[1]]
        return jnp.concatenate(
            [ref[r * off[0] + off[1], 0:hr], ref[l * off[0] + off[1], hr:s]], axis=0)

    def outputs(q, step, k):
        r, l = RING[step]

        def gated(e, cs):
            n = cs * el + e
            w = wv[q * CORES * el + n] if q < DIRECT else wb[(q - DIRECT) * CORES * el + n]
            o = jnp.dot(halves(ab, r, l, (CORES * el, n)), w,
                        preferred_element_type=jnp.float32)
            o = o.astype(jnp.bfloat16).astype(jnp.float32)
            col = jnp.sum(jnp.where(lane == n, halves(gb, r, l, (1, 0)), 0.0), axis=1, keepdims=True)
            return jnp.where(col != 0.0, o * col, 0.0)

        part[k] = jnp.zeros((s, CHUNK), jnp.float32)

        def more(e, _):
            part[k] = part[k] + (gated(e, 0) + gated(e, 1))
            return 0
        lax.fori_loop(0, el, more, 0)

    def ring(q, step, k):
        return (remote(part.at[k, lo], rb.at[0, q, step], rs_snd.at[0, q, step], rs_rcv.at[0, q, step], right),
                remote(part.at[k, hi], rb.at[1, q, step], rs_snd.at[1, q, step], rs_rcv.at[1, q, step], left))

    def add_arrived(q, step, k):
        for copy in ring(q, step - 1, k):
            copy.wait_recv()
        return (part[k, 0:hr] + rb[0, q, step - 1], part[k, hr:s] + rb[1, q, step - 1])

    sent = []

    def hop(q, step):
        n = len(sent)
        k = n % SLOTS
        if n >= SLOTS:
            for copy in sent[n - SLOTS]:
                copy.wait_send()
        outputs(q, step, k)
        if step:
            top, bottom = add_arrived(q, step, k)
            part[k, 0:hr] = top
            part[k, hr:s] = bottom
        sent.append(ring(q, step, k))
        for copy in sent[-1]:
            copy.start()

    def finish(q):
        outputs(q, 3, SLOTS)
        top, bottom = add_arrived(q, 3, SLOTS)
        cols = pl.ds(q * CHUNK, CHUNK)
        y_ref[0:hr, cols] = top.astype(y_ref.dtype)
        y_ref[hr:s, cols] = bottom.astype(y_ref.dtype)

    def prologue():
        gates_out()
        for e in range(el):
            w1_own(e).wait()
            w1_copy(2, e).wait_recv()
        x_own.wait()
        hiddens(0, 1, 0, el, 0, 1)

    def first_halves():
        cx_copy(0).wait_recv()
        cx_copy(2).wait_recv()
        cx_copy(4).start()
        cx_copy(5).start()

    def seconds():
        cx_copy(1).wait_recv()
        cx_copy(3).wait_recv()

    def opposite():
        cx_copy(4).wait_recv()
        cx_copy(5).wait_recv()

    def chunk(q, step):
        if step == 0:
            loaded(q)
        hop(q, step)

    seen = set()

    def need(*key):
        if key not in seen:
            seen.add(key)
            arrived(w1_copy, key[:2], key[2])

    def units(b0, n, e0, e1, far_slice):
        if b0:
            once(seconds)
        if b0 == 3:
            once(opposite)
        for e in range(e0, e1):
            need(*((7, 8) if far_slice else (5, 6)), e)
        hiddens(b0, n, e0, e1, *((3, 4) if far_slice else (0 if b0 else 1, 3)))

    def once(fn):
        if fn not in seen:
            seen.add(fn)
            fn()

    run = {
        "N1": lambda e: near(w1_copy, e), "F1": lambda e: far(w1_copy, e),
        "X1": first_halves, "X2": lambda: once(seconds), "X3": lambda: once(opposite),
        "G": gates_in, "H": units,
        "W": lambda q: start(w2_copy, (0, 1, 2), q),
        "N2": lambda q: near(w2_copy, q), "F2": lambda q: far(w2_copy, q), "L": load,
        "R": chunk, "E": finish,
    }
    prologue()
    for op, *args in PROGRAM:
        run[op](*args)

    for copies in sent[-SLOTS:]:
        for copy in copies:
            copy.wait_send()
    for kind in range(6):
        cx_copy(kind).wait_send()
    for kind in range(3):
        g_copy(kind).wait_send()
    for kind in range(9):
        for q in range(nq):
            w2_copy(kind, q).wait_send()


def solution(mesh):
    ntp = mesh.shape["tp"]
    nep = mesh.shape["ep"]
    nx = nep // CORES

    def body(x, idx, gates, w1, w2):
        t_n, h = x.shape
        el, fs = w1.shape[0], w1.shape[2]
        n_exp = el * nep
        k = idx.shape[1]
        s = t_n // ntp
        cap = 8 * ((5 * k * s + 32 * n_exp - 1) // (32 * n_exp))
        kb = ntp * fs
        nb = h // kb
        nq = h // CHUNK
        rows = -(-CORES * el // 8) * 8
        bf16, f32, dma = jnp.bfloat16, jnp.float32, pltpu.SemaphoreType.DMA
        any_space = pl.BlockSpec(memory_space=pl.ANY)
        y, _ = pl.pallas_call(
            functools.partial(kernel, ntp=ntp, nep=nep, cap=cap),
            out_shape=(jax.ShapeDtypeStruct((s, h), bf16),
                       jax.ShapeDtypeStruct(((nq - DIRECT) * CORES * el, kb, CHUNK), bf16)),
            in_specs=[any_space] * 5,
            out_specs=(pl.BlockSpec(memory_space=pltpu.VMEM), any_space),
            scratch_shapes=[
                pltpu.VMEM((4, s, h), bf16),
                pltpu.VMEM((k, s), jnp.int32),
                pltpu.VMEM((k, s), f32),
                pltpu.VMEM((nx, rows, s), f32),
                pltpu.VMEM((4, rows, s), f32),
                pltpu.VMEM((4, s, 128), f32),
                pltpu.VMEM((nq * CORES * el, kb, CHUNK), bf16),
                pltpu.VMEM((DIRECT * CORES * el, kb, CHUNK), bf16),
                pltpu.VMEM((4 * CORES * el, s, kb), bf16),
                pltpu.VMEM((2, nq, 3, s // 2, CHUNK), f32),
                pltpu.VMEM((SLOTS + 1, s, CHUNK), f32),
                dma((3,)), dma((6,)), dma((6,)), dma((3,)), dma((3,)), dma((el,)),
                dma((9, el)), dma((9, el)), dma((9, nq)), dma((9, nq)),
                dma((3, nq)), dma((2, nq, 3)), dma((2, nq, 3)),
            ],
            compiler_params=pltpu.CompilerParams(
                collective_id=0, has_side_effects=True, vmem_limit_bytes=67_000_000),
        )(x, idx.T, gates.T, w1.reshape(el, nb, kb, fs), w2)
        return y

    row = P(("dp", "ep"), None)
    return jax.shard_map(
        body,
        mesh=mesh,
        in_specs=(row, row, row, P("ep", None, "tp"), P("ep", "tp", None)),
        out_specs=P(("dp", "ep", "tp"), None),
        check_vma=False,
    )
```
